32 devices in a mesh: dp: 8 (over z, core), tile: 4 (over y, x).
Axes of the slice: x: 2, y: 2, z: 4, core: 2. Of those that a mesh axis runs over, the one named last changes fastest.
Arguments:
- features: bfloat16 [8, 256, 512], P('dp', 'tile'), may hold values from -6 to 6
- depth_probs: float32 [8, 256, 118], P('dp', 'tile'), may hold values from 0 to 1, as said below
- context: bfloat16 [8, 256, 80], P('dp', 'tile'), may hold values from -2 to 2
- bev_grad: bfloat16 [8, 10240, 80], P('dp', 'tile'), may hold values from -18 to 18
- head_weight: bfloat16 [198, 512], replicated, may hold values from -0.4375 to 0.4375
- slot_cell: int32 [8, 4, 4, 512], P('dp', 'tile'), may hold values from 0 to 2559, as said below
- slot_point: int32 [8, 4, 4, 512], P('dp', 'tile'), may hold values from 0 to 7551, as said below
- slot_count: int32 [8, 4, 4], P('dp'), may hold values from 1 to 512, as said below
Outputs:
- grad_features: bfloat16 [8, 256, 512], P('dp', 'tile')
- head_weight_grad: float32 [512, 198], P('tile')
The draws below stay inside these ranges and needn't reach their ends.
Inputs may be any that keep to these rules, and one draw needn't show every extreme that they name: `slot_count`: every block holds at most 512 live slots; in every scene group one tile receives exactly 512 from every device; the live slots of one device and group sum to at most 7552. `slot_point`: A live slot names a point of the sending device; within one group and sending device each point is named by at most one live slot; dead slots hold 0. `slot_cell`: A live slot names a cell of the receiving tile; dead slots hold 0. `depth_probs`: each pixel's 118 entries are positive and sum to one.
All inputs are finite; a program needn't handle non-finite values.
Results may differ from the reference program's by a relative error of at most 0.0049.
Values may be sent and summed in bfloat16 or wider, within the bound.
A program may use at most 64 MiB of HBM per device.

```python
import jax
import jax.numpy as jnp
from jax import lax

C = 80
DB = 118
FEAT = 512
PIX_DEV = 64
CELLS_DEV = 2560
CAP = 512
GROUPS = 8
TILES = 4
PIXELS = 256
BEV_CELLS = 10240
HEAD = 198


def table_counts(key):
    base_key = jax.random.fold_in(key, 11)
    hot_tile = jax.random.randint(jax.random.fold_in(base_key, 1), (GROUPS,), 0, TILES)
    spread = jax.random.randint(jax.random.fold_in(base_key, 2), (GROUPS, TILES, TILES), CAP // 4, CAP // 2 + 1)
    dest_ids = jnp.arange(TILES, dtype=jnp.int32)
    return jnp.where(dest_ids[None, None, :] == hot_tile[:, None, None], CAP, spread).astype(jnp.int32)


def draw_slot_count(key, part):
    return table_counts(key)


def shuffle_one(perm_key):
    return jax.random.permutation(perm_key, PIX_DEV * DB).astype(jnp.int32)


def draw_slot_point(key, part):
    counts = table_counts(key)
    point_total = PIX_DEV * DB
    perm_keys = jax.random.split(jax.random.fold_in(key, 23), GROUPS * TILES)
    shuffled = jax.vmap(shuffle_one)(perm_keys).reshape(GROUPS, TILES, point_total)
    offsets = jnp.cumsum(counts, axis=-1) - counts
    slot_ids = jnp.arange(CAP, dtype=jnp.int32)
    position = jnp.minimum(offsets[..., None] + slot_ids, point_total - 1).astype(jnp.int32)
    picked = jnp.take_along_axis(shuffled, position.reshape(GROUPS, TILES, TILES * CAP), axis=-1)
    picked = picked.reshape(GROUPS, TILES, TILES, CAP)
    return jnp.where(slot_ids < counts[..., None], picked, 0).astype(jnp.int32)


def draw_slot_cell(key, part):
    counts = table_counts(key)
    cells = jax.random.randint(jax.random.fold_in(key, 37), (GROUPS, TILES, TILES, CAP), 0, CELLS_DEV)
    slot_ids = jnp.arange(CAP, dtype=jnp.int32)
    cells = jnp.where(slot_ids < counts[..., None], cells, 0)
    return jnp.transpose(cells, (0, 2, 1, 3)).astype(jnp.int32)


def draw_depth_probs(key, part):
    logits = 0.3 * jax.random.normal(key, (GROUPS, PIXELS, DB), jnp.float32)
    return jax.nn.softmax(logits, axis=-1).astype(jnp.float32)


def spiked(result, rng, source, target, shards_of, factor):
    def block_of(dim):
        return (jnp.arange(result.shape[dim]) // (result.shape[dim] // shards_of)).reshape((-1,) + (1,) * (result.ndim - 1 - dim))

    one_side = jax.random.permutation(rng, shards_of)[block_of(target)]
    second = (block_of(target) + shards_of // 2) % shards_of
    return jnp.where((block_of(source) == one_side) | (block_of(source) == second), factor * result, result)


def block_scale(stream_key, extent, pieces, smallest, high):
    loudness, own = 1.0, jax.random.fold_in(stream_key, 6)
    for axis_at, shards_of in pieces:
        steps = jnp.exp(jax.random.uniform(jax.random.fold_in(own, axis_at), (shards_of,), jnp.float32, smallest / len(pieces), high / len(pieces)))
        loudness = loudness * jnp.repeat(steps, extent[axis_at] // shards_of).reshape([-1 if axis == axis_at else 1 for axis in range(len(extent))])
    return loudness


def normal_values(own_key, dims, scale, most, cuts=(), kind=jnp.bfloat16):
    gain = block_scale(own_key, dims, cuts, -0.22, 0.18) if cuts else 1.0
    result = jax.random.normal(own_key, dims, jnp.float32) * scale * gain
    return jnp.minimum(jnp.maximum(result, -most), most).astype(kind)


def noise_with(rng, dims, scale, bound, cuts, heavy, kind=jnp.bfloat16):
    drawn = scale * jax.random.normal(rng, dims, jnp.float32)
    if cuts:
        drawn = drawn * block_scale(rng, dims, cuts, -0.22, 0.18)
    return jnp.clip(spiked(drawn, jax.random.fold_in(rng, 3), *heavy), -bound, bound).astype(kind)


def setup_inputs(seed: int = 0) -> dict:
    splits = jax.random.split(jax.random.key(seed), 9)
    return {
        "features": noise_with(splits[0], (GROUPS, PIXELS, FEAT), 1.0, 6.0, ((0, 8), (1, 4)), (1, 2, 4, 2.0)),
        "depth_probs": draw_depth_probs(jax.random.fold_in(splits[8], 71), 0),
        "context": normal_values(splits[2], (GROUPS, PIXELS, C), 0.3, 2.0, ((0, 8), (1, 4))),
        "bev_grad": normal_values(splits[3], (GROUPS, BEV_CELLS, C), 3.0, 18.0, ((0, 8), (1, 4))),
        "head_weight": normal_values(splits[4], (HEAD, FEAT), HEAD ** -0.5, 0.4375),
        "slot_cell": draw_slot_cell(jax.random.fold_in(splits[8], 71), 0),
        "slot_point": draw_slot_point(jax.random.fold_in(splits[8], 71), 0),
        "slot_count": draw_slot_count(jax.random.fold_in(splits[8], 71), 0),
    }


def one_group(features, depth_probs, context, bev_grad, slot_cell, slot_point, slot_count, head_weight):
    tile_count = slot_count.shape[0]
    cell_by_src = jnp.transpose(slot_cell, (1, 0, 2))
    tile_ids = jnp.arange(tile_count, dtype=jnp.int32)
    global_cell = cell_by_src + (tile_ids * CELLS_DEV).astype(jnp.int32)[None, :, None]
    global_point = slot_point + (tile_ids * (PIX_DEV * DB)).astype(jnp.int32)[:, None, None]
    live_slots = jnp.arange(CAP, dtype=jnp.int32)[None, None, :] < slot_count[:, :, None]
    looked_up = bev_grad[global_cell.reshape(-1)].reshape(tile_count, tile_count, CAP, C)
    looked_up = jnp.where(live_slots[..., None], looked_up, jnp.zeros((), bev_grad.dtype))
    point_grads = jnp.zeros((tile_count * PIX_DEV * DB, C), bev_grad.dtype)
    point_grads = point_grads.at[global_point.reshape(-1)].add(looked_up.reshape(-1, C))
    point_grads = point_grads.reshape(tile_count * PIX_DEV, DB, C).astype(jnp.float32)
    context32 = context.astype(jnp.float32)
    grad_depth = jnp.einsum('pdc,pc->pd', point_grads, context32, precision=lax.Precision.HIGHEST)
    grad_ctx = jnp.einsum('pd,pdc->pc', depth_probs, point_grads, precision=lax.Precision.HIGHEST)
    grad_logits = depth_probs * (grad_depth - jnp.sum(depth_probs * grad_depth, axis=-1, keepdims=True))
    head_grad = jnp.concatenate([grad_logits, grad_ctx], axis=-1).astype(jnp.bfloat16)
    grad_feats = jnp.dot(head_grad, head_weight, preferred_element_type=jnp.float32).astype(jnp.bfloat16)
    weight_term = jnp.dot(features.T, head_grad, preferred_element_type=jnp.float32)
    return grad_feats, weight_term


def reference(features, depth_probs, context, bev_grad, head_weight, slot_cell, slot_point, slot_count):
    def accumulate(summed, group_items):
        grad_feats, weight_term = one_group(*group_items, head_weight)
        return summed + weight_term, grad_feats

    initial = jnp.zeros((FEAT, DB + C), jnp.float32)
    summed, grad_feats = lax.scan(accumulate, initial, (features, depth_probs, context, bev_grad, slot_cell, slot_point, slot_count))
    return grad_feats, summed
```

```python
import functools

import jax
import jax.numpy as jnp
from jax import lax
from jax.experimental import pallas as pl
from jax.experimental.pallas import tpu as pltpu
from jax.sharding import PartitionSpec as P

F32 = jnp.float32
BF16 = jnp.bfloat16
MESH = pl.DeviceIdType.MESH
LANES = 128


def dot(a, b):
    return lax.dot_general(a, b, (((1,), (0,)), ((), ())), preferred_element_type=F32)


def dot_nt(a, b):
    return lax.dot_general(a, b, (((1,), (1,)), ((), ())), preferred_element_type=F32)


def eye(n):
    rows = lax.broadcasted_iota(jnp.int32, (n, n), 0)
    cols = lax.broadcasted_iota(jnp.int32, (n, n), 1)
    return (rows == cols).astype(BF16)


def transposed(x):
    return dot_nt(eye(x.shape[1]), x)


def kernel(
    dims,
    counts_ref,
    feat_ref,
    probs_ref,
    ctx_ref,
    bev_t,
    weight_ref,
    cell_ref,
    point_ref,
    gfeat_ref,
    gweight_ref,
    out_val,
    in_val,
    head_t,
    own_half,
    core_out,
    core_in,
    tile_out,
    tile_in,
    z_out,
    z_in,
    fin_out,
    fin_in,
    val_send,
    val_recv,
    core_send,
    core_recv,
    tile_send,
    tile_recv,
    z_send,
    z_recv,
    fin_send,
    fin_recv,
):
    tiles, pairs, half = dims
    me = lax.axis_index("tile")
    dp = lax.axis_index("dp")
    zi = dp // 2
    core = dp - zi * 2
    partner = zi * 2 + 1 - core

    def tile_peer(j):
        return (dp, lax.rem(me + j, tiles))

    def z_peer(j):
        return (lax.rem(zi + j, pairs) * 2 + core, me)

    barrier = pltpu.get_barrier_semaphore()
    for j in range(1, tiles):
        pl.semaphore_signal(barrier, inc=1, device_id=tile_peer(j), device_id_type=MESH)
    for j in range(1, pairs):
        pl.semaphore_signal(barrier, inc=1, device_id=z_peer(j), device_id_type=MESH)
    pl.semaphore_signal(barrier, inc=1, device_id=(partner, me), device_id_type=MESH)

    channels, cells = bev_t.shape
    cap = cell_ref.shape[1]
    pixels, bins = probs_ref.shape
    chunk = 512 if cells % 512 == 0 else cells
    lane = lax.broadcasted_iota(jnp.int32, (1, cap), 1)

    def lookup(j):
        dest = lax.rem(me + j, tiles)
        row = cell_ref[pl.ds(dest, 1), :]
        row = jnp.where(lane < counts_ref[dest, me], row, -1)
        total = jnp.zeros((channels, cap), F32)
        rows = lax.broadcasted_iota(jnp.int32, (chunk, cap), 0)
        for lo in range(0, cells, chunk):
            hot = (rows == row - lo).astype(BF16)
            total += dot(bev_t[:, lo : lo + chunk], hot)
        return total.astype(BF16)

    val_copies = []
    for j in range(1, tiles):
        out_val[j - 1] = lookup(j)
        if j == 1:
            pl.semaphore_wait(barrier, tiles + pairs - 1)
        copy = pltpu.make_async_remote_copy(
            src_ref=out_val.at[j - 1],
            dst_ref=in_val.at[j - 1],
            send_sem=val_send.at[j - 1],
            recv_sem=val_recv.at[j - 1],
            device_id=tile_peer(j),
            device_id_type=MESH,
        )
        copy.start()
        val_copies.append(copy)
    own_val = lookup(0)

    ctx_t = transposed(ctx_ref[...]).astype(BF16)
    probs = probs_ref[...]
    probs_hi = probs.astype(BF16)
    probs_lo = (probs - probs_hi.astype(F32)).astype(BF16)
    probs_hi_t = transposed(probs_hi)
    probs_t = probs_hi_t + transposed(probs_lo)
    probs_bt = probs_hi_t.astype(BF16)
    grad_depth = jnp.zeros((bins, pixels), F32)
    grad_ctx = jnp.zeros((channels, pixels), F32)
    pixel_rows = lax.broadcasted_iota(jnp.int32, (pixels, cap), 0)
    bin_rows = lax.broadcasted_iota(jnp.int32, (bins, cap), 0)
    for j in range(tiles):
        source = lax.rem(me + tiles - j, tiles)
        point = point_ref[pl.ds(source, 1), :].astype(F32)
        pixel = jnp.floor((point + 0.5) * (1.0 / bins))
        bin_of = (point - pixel * bins).astype(jnp.int32)
        pixel_hot = (pixel_rows == pixel.astype(jnp.int32)).astype(BF16)
        bin_hot = bin_rows == bin_of
        ctx_slot = dot(ctx_t, pixel_hot)
        prob_slot = jnp.sum(
            jnp.where(bin_hot, dot(probs_bt, pixel_hot), 0.0), axis=0, keepdims=True
        )
        if j:
            val_copies[j - 1].wait_recv()
            values = in_val[j - 1].astype(F32)
        else:
            values = own_val.astype(F32)
        slot_grad = jnp.sum(values * ctx_slot, axis=0, keepdims=True)
        spread = jnp.where(bin_hot, slot_grad, 0.0).astype(BF16)
        grad_depth += dot_nt(spread, pixel_hot)
        grad_ctx += dot_nt((values * prob_slot).astype(BF16), pixel_hot)

    mean = jnp.sum(probs_t * grad_depth, axis=0, keepdims=True)
    head_t[...] = jnp.zeros_like(head_t)
    head_t[0:bins, :] = probs_t * (grad_depth - mean)
    head_t[bins : bins + channels, :] = grad_ctx

    feats = feat_ref[...]
    share = feats.shape[1] // tiles
    other_head = head_t[pl.ds(pl.multiple_of((1 - core) * half, 8), half), :].astype(BF16)
    own_head = head_t[pl.ds(pl.multiple_of(core * half, 8), half), :].astype(BF16)
    product = dot(other_head, feats)
    for t in range(tiles):
        core_out[t] = product[:, t * share : (t + 1) * share].astype(BF16)
    core_copy = pltpu.make_async_remote_copy(
        src_ref=core_out,
        dst_ref=core_in,
        send_sem=core_send,
        recv_sem=core_recv,
        device_id=(partner, me),
        device_id_type=MESH,
    )
    core_copy.start()
    product = dot(own_head, feats)
    for t in range(tiles):
        own_half[t] = product[:, t * share : (t + 1) * share]
    core_copy.wait_recv()

    tile_copies = []
    for j in range(1, tiles):
        dest = lax.rem(me + j, tiles)
        tile_out[j - 1] = (own_half[dest] + core_in[dest].astype(F32)).astype(BF16)
        copy = pltpu.make_async_remote_copy(
            src_ref=tile_out.at[j - 1],
            dst_ref=tile_in.at[j - 1],
            send_sem=tile_send.at[j - 1],
            recv_sem=tile_recv.at[j - 1],
            device_id=tile_peer(j),
            device_id_type=MESH,
        )
        copy.start()
        tile_copies.append(copy)
    total = own_half[me] + core_in[me].astype(F32)

    head = dot_nt(eye(pixels), head_t[...].astype(BF16)).astype(BF16)
    outputs = bins + channels
    gfeat_ref[...] = dot(head[:, :outputs], weight_ref[...]).astype(BF16)

    for j in range(1, tiles):
        tile_copies[j - 1].wait_recv()
        total += tile_in[j - 1].astype(F32)
    z_copies = []
    z_out[...] = total.astype(BF16)
    for j in range(1, pairs):
        copy = pltpu.make_async_remote_copy(
            src_ref=z_out,
            dst_ref=z_in.at[j - 1],
            send_sem=z_send.at[j - 1],
            recv_sem=z_recv.at[j - 1],
            device_id=z_peer(j),
            device_id_type=MESH,
        )
        copy.start()
        z_copies.append(copy)
    for j in range(1, pairs):
        z_copies[j - 1].wait_recv()
        total += z_in[j - 1].astype(F32)
    fin_out[...] = total
    fin_copy = pltpu.make_async_remote_copy(
        src_ref=fin_out,
        dst_ref=fin_in,
        send_sem=fin_send,
        recv_sem=fin_recv,
        device_id=(partner, me),
        device_id_type=MESH,
    )
    fin_copy.start()
    gweight_ref[pl.ds(pl.multiple_of(core * half, 8), half), :] = total
    for copy in val_copies + [core_copy] + tile_copies + z_copies:
        copy.wait_send()
    fin_copy.wait()
    gweight_ref[pl.ds(pl.multiple_of((1 - core) * half, 8), half), :] = fin_in[...]


def body(tiles, dps, features, depth_probs, context, bev_grad, head_weight, slot_cell, slot_point, slot_count):
    features = features[0]
    depth_probs = depth_probs[0]
    context = context[0]
    bev_t = bev_grad[0].T
    cell_table = slot_cell[0, 0]
    points = slot_point[0, 0]
    counts = slot_count[0]
    cap = cell_table.shape[1]
    pixels, bins = depth_probs.shape
    channels = context.shape[1]
    inputs = features.shape[1]
    outputs = bins + channels
    pairs = dps // 2
    share = inputs // tiles
    half = -(-outputs // 32) * 16
    vmem = pl.BlockSpec(memory_space=pltpu.VMEM)
    dma = pltpu.SemaphoreType.DMA
    grad_feats, weight_t = pl.pallas_call(
        functools.partial(kernel, (tiles, pairs, half)),
        out_shape=(
            jax.ShapeDtypeStruct((pixels, inputs), BF16),
            jax.ShapeDtypeStruct((2 * half, share), F32),
        ),
        in_specs=[pl.BlockSpec(memory_space=pltpu.SMEM)] + [vmem] * 7,
        out_specs=(vmem, vmem),
        scratch_shapes=[
            pltpu.VMEM((tiles - 1, channels, cap), BF16),
            pltpu.VMEM((tiles - 1, channels, cap), BF16),
            pltpu.VMEM((2 * half, pixels), F32),
            pltpu.VMEM((tiles, half, share), F32),
            pltpu.VMEM((tiles, half, share), BF16),
            pltpu.VMEM((tiles, half, share), BF16),
            pltpu.VMEM((tiles - 1, half, share), BF16),
            pltpu.VMEM((tiles - 1, half, share), BF16),
            pltpu.VMEM((half, share), BF16),
            pltpu.VMEM((pairs - 1, half, share), BF16),
            pltpu.VMEM((half, share), F32),
            pltpu.VMEM((half, share), F32),
            dma((tiles - 1,)),
            dma((tiles - 1,)),
            dma,
            dma,
            dma((tiles - 1,)),
            dma((tiles - 1,)),
            dma((pairs - 1,)),
            dma((pairs - 1,)),
            dma,
            dma,
        ],
        compiler_params=pltpu.CompilerParams(collective_id=0, has_side_effects=True),
        name="splat_backward",
    )(counts, features, depth_probs, context, bev_t, head_weight, cell_table, points)
    return (grad_feats[None], weight_t[:outputs].T)


def solution(mesh):
    return jax.shard_map(
        functools.partial(body, mesh.shape["tile"], mesh.shape["dp"]),
        mesh=mesh,
        in_specs=(
            P("dp", "tile", None),
            P("dp", "tile", None),
            P("dp", "tile", None),
            P("dp", "tile", None),
            P(),
            P("dp", "tile", None, None),
            P("dp", "tile", None, None),
            P("dp", None, None),
        ),
        out_specs=(P("dp", "tile", None), P("tile", None)),
        check_vma=False,
    )
```

```python
import functools

import jax
import jax.numpy as jnp
from jax import lax
from jax.experimental import pallas as pl
from jax.experimental.pallas import tpu as pltpu
from jax.sharding import PartitionSpec as P

F32 = jnp.float32
BF16 = jnp.bfloat16
MESH = pl.DeviceIdType.MESH


def dot(a, b):
    return lax.dot_general(a, b, (((1,), (0,)), ((), ())), preferred_element_type=F32)


def dot_nt(a, b):
    return lax.dot_general(a, b, (((1,), (1,)), ((), ())), preferred_element_type=F32)


def eye(n):
    rows = lax.broadcasted_iota(jnp.int32, (n, n), 0)
    cols = lax.broadcasted_iota(jnp.int32, (n, n), 1)
    return (rows == cols).astype(BF16)


def transposed(x):
    return dot_nt(eye(x.shape[1]), x)


def kernel(
    dims,
    counts_hbm,
    feat_hbm,
    probs_hbm,
    ctx_hbm,
    bev_hbm,
    weight_hbm,
    cell_hbm,
    point_hbm,
    gfeat_ref,
    gweight_ref,
    counts_ref,
    feat_ref,
    probs_ref,
    ctx_ref,
    bev_t,
    weight_ref,
    cell_ref,
    point_ref,
    out_val,
    in_val,
    head_t,
    own_half,
    core_out,
    core_in,
    tile_out,
    tile_in,
    z_out,
    z_in,
    fin_out,
    fin_in,
    load_sem,
    val_send,
    val_recv,
    core_send,
    core_recv,
    tile_send,
    tile_recv,
    z_send,
    z_recv,
    fin_send,
    fin_recv,
    up_sem,
    down_sem,
):
    tiles, pairs, half = dims
    me = lax.axis_index("tile")
    dp = lax.axis_index("dp")
    zi = dp // 2
    core = dp - zi * 2
    partner = zi * 2 + 1 - core
    order = sorted(range(1, tiles), key=lambda j: -bin(j).count("1"))

    def flipped(j):
        index = 0
        for place in range(tiles.bit_length() - 1):
            bit = lax.rem(me // 2**place, 2)
            index = index + 2**place * ((1 - bit) if (j >> place) & 1 else bit)
        return index

    def tile_peer(j):
        return (dp, flipped(j))

    def z_peer(j):
        return (lax.rem(zi + j, pairs) * 2 + core, me)

    def z_step(by):
        return ((zi + by) * 2 + core, me)

    def signal(sem, device):
        pl.semaphore_signal(sem, inc=1, device_id=device, device_id_type=MESH)

    barrier = pltpu.get_barrier_semaphore()
    for j in order:
        signal(barrier, tile_peer(j))
    signal(barrier, (partner, me))

    @pl.when(zi > 0)
    def _():
        signal(barrier, z_step(-1))

    @pl.when(zi < pairs - 1)
    def _():
        signal(barrier, z_step(1))

    loads = []
    sources = (cell_hbm, counts_hbm, bev_hbm, point_hbm, ctx_hbm, probs_hbm, feat_hbm, weight_hbm)
    targets = (cell_ref, counts_ref, bev_t, point_ref, ctx_ref, probs_ref, feat_ref, weight_ref)
    for at, (src, dst) in enumerate(zip(sources, targets)):
        load = pltpu.make_async_copy(src, dst, load_sem.at[at])
        load.start()
        loads.append(load)

    def token_send(k):
        @pl.when((zi < pairs - 1) & (zi >= k))
        def _():
            signal(up_sem.at[k - 1], z_step(1))

        @pl.when((zi > 0) & (zi + k < pairs))
        def _():
            signal(down_sem.at[k - 1], z_step(-1))

    def token_wait(k):
        @pl.when(zi > k)
        def _():
            pl.semaphore_wait(up_sem.at[k - 1], 1)

        @pl.when(zi + k + 1 < pairs)
        def _():
            pl.semaphore_wait(down_sem.at[k - 1], 1)

    channels, cells = bev_t.shape
    cap = cell_ref.shape[1]
    pixels, bins = probs_ref.shape
    chunk = 512 if cells % 512 == 0 else cells
    lane = lax.broadcasted_iota(jnp.int32, (1, cap), 1)
    tile_lane = lax.broadcasted_iota(jnp.int32, (1, tiles), 1)

    def lookup(j):
        dest = flipped(j)
        row = cell_ref[pl.ds(dest, 1), :]
        live = jnp.sum(
            jnp.where(tile_lane == me, counts_ref[pl.ds(dest, 1), :], 0), axis=1, keepdims=True
        )
        row = jnp.where(lane < live, row, -1)
        total = jnp.zeros((channels, cap), F32)
        rows = lax.broadcasted_iota(jnp.int32, (chunk, cap), 0)
        for lo in range(0, cells, chunk):
            hot = (rows == row - lo).astype(BF16)
            total += dot(bev_t[:, lo : lo + chunk], hot)
        return total.astype(BF16)

    for load in loads[:3]:
        load.wait()
    val_copies = {
        j: pltpu.make_async_remote_copy(
            src_ref=out_val.at[j - 1],
            dst_ref=in_val.at[j - 1],
            send_sem=val_send.at[j - 1],
            recv_sem=val_recv.at[j - 1],
            device_id=tile_peer(j),
            device_id_type=MESH,
        )
        for j in order
    }
    early = order[:2]
    for j in early:
        out_val[j - 1] = lookup(j)

    beside = jnp.minimum(zi, 1) + jnp.minimum(pairs - 1 - zi, 1)
    pl.semaphore_wait(barrier, tiles + beside)
    for j in early:
        val_copies[j].start()
    if pairs > 2:
        token_send(1)
    for j in order[2:]:
        out_val[j - 1] = lookup(j)
        val_copies[j].start()
    own_val = lookup(0)

    for load in loads[3:]:
        load.wait()
    ctx_t = transposed(ctx_ref[...]).astype(BF16)
    probs = probs_ref[...]
    probs_hi = probs.astype(BF16)
    probs_lo = (probs - probs_hi.astype(F32)).astype(BF16)
    probs_hi_t = transposed(probs_hi)
    probs_t = probs_hi_t + transposed(probs_lo)
    probs_bt = probs_hi_t.astype(BF16)
    grad_depth = jnp.zeros((bins, pixels), F32)
    grad_ctx = jnp.zeros((channels, pixels), F32)
    pixel_rows = lax.broadcasted_iota(jnp.int32, (pixels, cap), 0)
    bin_rows = lax.broadcasted_iota(jnp.int32, (bins, cap), 0)
    arrivals = [0] + order[::-1]
    tables = {}
    for j in arrivals:
        point = point_ref[pl.ds(flipped(j), 1), :].astype(F32)
        pixel = jnp.floor((point + 0.5) * (1.0 / bins))
        bin_of = (point - pixel * bins).astype(jnp.int32)
        pixel_hot = (pixel_rows == pixel.astype(jnp.int32)).astype(BF16)
        ctx_slot = dot(ctx_t, pixel_hot)
        prob_slot = jnp.sum(
            jnp.where(bin_rows == bin_of, dot(probs_bt, pixel_hot), 0.0), axis=0, keepdims=True
        )
        tables[j] = (bin_of, pixel_hot, ctx_slot, prob_slot)
    for j in arrivals:
        bin_of, pixel_hot, ctx_slot, prob_slot = tables[j]
        if j:
            val_copies[j].wait_recv()
            values = in_val[j - 1].astype(F32)
        else:
            values = own_val.astype(F32)
        slot_grad = jnp.sum(values * ctx_slot, axis=0, keepdims=True)
        spread = jnp.where(bin_rows == bin_of, slot_grad, 0.0).astype(BF16)
        grad_depth += dot_nt(spread, pixel_hot)
        grad_ctx += dot_nt((values * prob_slot).astype(BF16), pixel_hot)

    mean = jnp.sum(probs_t * grad_depth, axis=0, keepdims=True)
    head_t[...] = jnp.zeros_like(head_t)
    head_t[0:bins, :] = probs_t * (grad_depth - mean)
    head_t[bins : bins + channels, :] = grad_ctx

    feats = feat_ref[...]
    share = feats.shape[1] // tiles
    other_head = head_t[pl.ds(pl.multiple_of((1 - core) * half, 8), half), :].astype(BF16)
    own_head = head_t[pl.ds(pl.multiple_of(core * half, 8), half), :].astype(BF16)
    product = dot(other_head, feats)
    for t in range(tiles):
        core_out[t] = product[:, t * share : (t + 1) * share].astype(BF16)
    core_copy = pltpu.make_async_remote_copy(
        src_ref=core_out,
        dst_ref=core_in,
        send_sem=core_send,
        recv_sem=core_recv,
        device_id=(partner, me),
        device_id_type=MESH,
    )
    core_copy.start()
    product = dot(own_head, feats)
    for t in range(tiles):
        own_half[t] = product[:, t * share : (t + 1) * share]
    core_copy.wait_recv()

    tile_copies = []
    for j in order:
        dest = flipped(j)
        tile_out[j - 1] = (own_half[dest] + core_in[dest].astype(F32)).astype(BF16)
        copy = pltpu.make_async_remote_copy(
            src_ref=tile_out.at[j - 1],
            dst_ref=tile_in.at[j - 1],
            send_sem=tile_send.at[j - 1],
            recv_sem=tile_recv.at[j - 1],
            device_id=tile_peer(j),
            device_id_type=MESH,
        )
        copy.start()
        tile_copies.append(copy)
    total = own_half[me] + core_in[me].astype(F32)

    head = dot_nt(eye(pixels), head_t[...].astype(BF16)).astype(BF16)
    outputs = bins + channels
    gfeat_ref[...] = dot(head[:, :outputs], weight_ref[...]).astype(BF16)

    for k in range(1, pairs - 1):
        token_wait(k)
        if k < pairs - 2:
            token_send(k + 1)
    for at in reversed(range(tiles - 1)):
        tile_copies[at].wait_recv()
        total += tile_in[order[at] - 1].astype(F32)
    z_copies = []
    z_out[...] = total.astype(BF16)
    for j in range(1, pairs):
        copy = pltpu.make_async_remote_copy(
            src_ref=z_out,
            dst_ref=z_in.at[j - 1],
            send_sem=z_send.at[j - 1],
            recv_sem=z_recv.at[j - 1],
            device_id=z_peer(j),
            device_id_type=MESH,
        )
        copy.start()
        z_copies.append(copy)
    for j in range(1, pairs):
        z_copies[j - 1].wait_recv()
        total += z_in[j - 1].astype(F32)
    fin_out[...] = total
    fin_copy = pltpu.make_async_remote_copy(
        src_ref=fin_out,
        dst_ref=fin_in,
        send_sem=fin_send,
        recv_sem=fin_recv,
        device_id=(partner, me),
        device_id_type=MESH,
    )
    fin_copy.start()
    for copy in list(val_copies.values()) + [core_copy] + tile_copies + z_copies:
        copy.wait_send()
    fin_copy.wait()
    other = fin_in[...]
    first = core == 0
    gweight_ref[0:half, :] = jnp.where(first, total, other)
    gweight_ref[half:, :] = jnp.where(first, other, total)[: gweight_ref.shape[0] - half]


def body(tiles, dps, features, depth_probs, context, bev_grad, head_weight, slot_cell, slot_point, slot_count):
    features = features[0]
    depth_probs = depth_probs[0]
    context = context[0]
    bev_t = bev_grad[0].T
    cell_table = slot_cell[0, 0]
    points = slot_point[0, 0]
    counts = slot_count[0]
    cap = cell_table.shape[1]
    pixels, bins = depth_probs.shape
    channels = context.shape[1]
    inputs = features.shape[1]
    outputs = bins + channels
    pairs = dps // 2
    share = inputs // tiles
    half = -(-outputs // 32) * 16
    operands = (counts, features, depth_probs, context, bev_t, head_weight, cell_table, points)
    vmem = pl.BlockSpec(memory_space=pltpu.VMEM)
    dma = pltpu.SemaphoreType.DMA
    grad_feats, weight_t = pl.pallas_call(
        functools.partial(kernel, (tiles, pairs, half)),
        out_shape=(
            jax.ShapeDtypeStruct((pixels, inputs), BF16),
            jax.ShapeDtypeStruct((outputs, share), F32),
        ),
        in_specs=[pl.BlockSpec(memory_space=pl.ANY)] * 8,
        out_specs=(vmem, vmem),
        scratch_shapes=[pltpu.VMEM(a.shape, a.dtype) for a in operands]
        + [
            pltpu.VMEM((tiles - 1, channels, cap), BF16),
            pltpu.VMEM((tiles - 1, channels, cap), BF16),
            pltpu.VMEM((2 * half, pixels), F32),
            pltpu.VMEM((tiles, half, share), F32),
            pltpu.VMEM((tiles, half, share), BF16),
            pltpu.VMEM((tiles, half, share), BF16),
            pltpu.VMEM((tiles - 1, half, share), BF16),
            pltpu.VMEM((tiles - 1, half, share), BF16),
            pltpu.VMEM((half, share), BF16),
            pltpu.VMEM((pairs - 1, half, share), BF16),
            pltpu.VMEM((half, share), F32),
            pltpu.VMEM((half, share), F32),
            dma((len(operands),)),
            dma((tiles - 1,)),
            dma((tiles - 1,)),
            dma,
            dma,
            dma((tiles - 1,)),
            dma((tiles - 1,)),
            dma((pairs - 1,)),
            dma((pairs - 1,)),
            dma,
            dma,
            pltpu.SemaphoreType.REGULAR((max(pairs - 2, 1),)),
            pltpu.SemaphoreType.REGULAR((max(pairs - 2, 1),)),
        ],
        compiler_params=pltpu.CompilerParams(collective_id=0, has_side_effects=True),
        name="splat_backward",
    )(*operands)
    return (grad_feats[None], weight_t.T)


def solution(mesh):
    return jax.shard_map(
        functools.partial(body, mesh.shape["tile"], mesh.shape["dp"]),
        mesh=mesh,
        in_specs=(
            P("dp", "tile", None),
            P("dp", "tile", None),
            P("dp", "tile", None),
            P("dp", "tile", None),
            P(),
            P("dp", "tile", None, None),
            P("dp", "tile", None, None),
            P("dp", None, None),
        ),
        out_specs=(P("dp", "tile", None), P("tile", None)),
        check_vma=False,
    )
```

```python
import functools

import jax
import jax.numpy as jnp
from jax import lax
from jax.experimental import pallas as pl
from jax.experimental.pallas import tpu as pltpu
from jax.sharding import PartitionSpec as P

F32 = jnp.float32
BF16 = jnp.bfloat16
MESH = pl.DeviceIdType.MESH


def dot(a, b):
    return lax.dot_general(a, b, (((1,), (0,)), ((), ())), preferred_element_type=F32)


def dot_nt(a, b):
    return lax.dot_general(a, b, (((1,), (1,)), ((), ())), preferred_element_type=F32)


def eye(n):
    rows = lax.broadcasted_iota(jnp.int32, (n, n), 0)
    cols = lax.broadcasted_iota(jnp.int32, (n, n), 1)
    return (rows == cols).astype(BF16)


def transposed(x):
    return dot_nt(eye(x.shape[1]), x)


def kernel(
    dims,
    counts_hbm,
    feat_hbm,
    probs_hbm,
    ctx_hbm,
    bev_hbm,
    weight_hbm,
    cell_hbm,
    point_hbm,
    gfeat_ref,
    gweight_ref,
    counts_ref,
    feat_ref,
    probs_ref,
    ctx_ref,
    bev_t,
    weight_ref,
    cell_ref,
    point_ref,
    out_val,
    in_val,
    head_t,
    own_half,
    core_out,
    core_in,
    tile_out,
    tile_in,
    z_out,
    z_in,
    fin_out,
    fin_in,
    load_sem,
    val_send,
    val_recv,
    core_send,
    core_recv,
    tile_send,
    tile_recv,
    z_send,
    z_recv,
    fin_send,
    fin_recv,
    up_sem,
    down_sem,
):
    tiles, pairs, half = dims
    me = lax.axis_index("tile")
    dp = lax.axis_index("dp")
    zi = dp // 2
    core = dp - zi * 2
    partner = zi * 2 + 1 - core
    order = sorted(range(1, tiles), key=lambda j: -bin(j).count("1"))

    def flipped(j):
        index = 0
        for place in range(tiles.bit_length() - 1):
            bit = lax.rem(me // 2**place, 2)
            index = index + 2**place * ((1 - bit) if (j >> place) & 1 else bit)
        return index

    def tile_peer(j):
        return (dp, flipped(j))

    def z_peer(j):
        return (lax.rem(zi + j, pairs) * 2 + core, me)

    def z_step(by):
        return ((zi + by) * 2 + core, me)

    def signal(sem, device):
        pl.semaphore_signal(sem, inc=1, device_id=device, device_id_type=MESH)

    barrier = pltpu.get_barrier_semaphore()
    for j in order:
        signal(barrier, tile_peer(j))
    signal(barrier, (partner, me))

    @pl.when(zi > 0)
    def _():
        signal(barrier, z_step(-1))

    @pl.when(zi < pairs - 1)
    def _():
        signal(barrier, z_step(1))

    loads = []
    sources = (cell_hbm, counts_hbm, bev_hbm, point_hbm, ctx_hbm, probs_hbm, feat_hbm, weight_hbm)
    targets = (cell_ref, counts_ref, bev_t, point_ref, ctx_ref, probs_ref, feat_ref, weight_ref)
    for at, (src, dst) in enumerate(zip(sources, targets)):
        load = pltpu.make_async_copy(src, dst, load_sem.at[at])
        load.start()
        loads.append(load)

    def token_send(k):
        @pl.when((zi < pairs - 1) & (zi >= k))
        def _():
            signal(up_sem.at[k - 1], z_step(1))

        @pl.when((zi > 0) & (zi + k < pairs))
        def _():
            signal(down_sem.at[k - 1], z_step(-1))

    def token_wait(k):
        @pl.when(zi > k)
        def _():
            pl.semaphore_wait(up_sem.at[k - 1], 1)

        @pl.when(zi + k + 1 < pairs)
        def _():
            pl.semaphore_wait(down_sem.at[k - 1], 1)

    channels, cells = bev_t.shape
    cap = cell_ref.shape[1]
    pixels, bins = probs_ref.shape
    chunk = 512 if cells % 512 == 0 else cells
    lane = lax.broadcasted_iota(jnp.int32, (1, cap), 1)
    tile_lane = lax.broadcasted_iota(jnp.int32, (1, tiles), 1)

    def lookup(j):
        dest = flipped(j)
        row = cell_ref[pl.ds(dest, 1), :]
        live = jnp.sum(
            jnp.where(tile_lane == me, counts_ref[pl.ds(dest, 1), :], 0), axis=1, keepdims=True
        )
        row = jnp.where(lane < live, row, -1)
        total = jnp.zeros((channels, cap), F32)
        rows = lax.broadcasted_iota(jnp.int32, (chunk, cap), 0)
        for lo in range(0, cells, chunk):
            hot = (rows == row - lo).astype(BF16)
            total += dot(bev_t[:, lo : lo + chunk], hot)
        return total.astype(BF16)

    for load in loads[:3]:
        load.wait()
    val_copies = {
        j: pltpu.make_async_remote_copy(
            src_ref=out_val.at[j - 1],
            dst_ref=in_val.at[j - 1],
            send_sem=val_send.at[j - 1],
            recv_sem=val_recv.at[j - 1],
            device_id=tile_peer(j),
            device_id_type=MESH,
        )
        for j in order
    }
    early = order[:1]
    for j in early:
        out_val[j - 1] = lookup(j)

    beside = jnp.minimum(zi, 1) + jnp.minimum(pairs - 1 - zi, 1)
    pl.semaphore_wait(barrier, tiles + beside)
    for j in early:
        val_copies[j].start()
    if pairs > 2:
        token_send(1)
    for j in order[1:]:
        out_val[j - 1] = lookup(j)
        val_copies[j].start()
    own_val = lookup(0)

    for load in loads[3:]:
        load.wait()
    ctx_t = transposed(ctx_ref[...]).astype(BF16)
    probs = probs_ref[...]
    probs_hi = probs.astype(BF16)
    probs_lo = (probs - probs_hi.astype(F32)).astype(BF16)
    probs_hi_t = transposed(probs_hi)
    probs_t = probs_hi_t + transposed(probs_lo)
    probs_bt = probs_hi_t.astype(BF16)
    grad_depth = jnp.zeros((bins, pixels), F32)
    grad_ctx = jnp.zeros((channels, pixels), F32)
    pixel_rows = lax.broadcasted_iota(jnp.int32, (pixels, cap), 0)
    bin_rows = lax.broadcasted_iota(jnp.int32, (bins, cap), 0)
    arrivals = [0] + order[::-1]
    tables = {}
    for j in arrivals:
        point = point_ref[pl.ds(flipped(j), 1), :].astype(F32)
        pixel = jnp.floor((point + 0.5) * (1.0 / bins))
        bin_of = (point - pixel * bins).astype(jnp.int32)
        pixel_hot = (pixel_rows == pixel.astype(jnp.int32)).astype(BF16)
        ctx_slot = dot(ctx_t, pixel_hot)
        prob_slot = jnp.sum(
            jnp.where(bin_rows == bin_of, dot(probs_bt, pixel_hot), 0.0), axis=0, keepdims=True
        )
        tables[j] = (bin_of, pixel_hot, ctx_slot, prob_slot)
    for j in arrivals:
        bin_of, pixel_hot, ctx_slot, prob_slot = tables[j]
        if j:
            val_copies[j].wait_recv()
            values = in_val[j - 1].astype(F32)
        else:
            values = own_val.astype(F32)
        slot_grad = jnp.sum(values * ctx_slot, axis=0, keepdims=True)
        spread = jnp.where(bin_rows == bin_of, slot_grad, 0.0).astype(BF16)
        grad_depth += dot_nt(spread, pixel_hot)
        grad_ctx += dot_nt((values * prob_slot).astype(BF16), pixel_hot)

    mean = jnp.sum(probs_t * grad_depth, axis=0, keepdims=True)
    head_t[...] = jnp.zeros_like(head_t)
    head_t[0:bins, :] = probs_t * (grad_depth - mean)
    head_t[bins : bins + channels, :] = grad_ctx

    feats = feat_ref[...]
    share = feats.shape[1] // tiles
    other_head = head_t[pl.ds(pl.multiple_of((1 - core) * half, 8), half), :].astype(BF16)
    own_head = head_t[pl.ds(pl.multiple_of(core * half, 8), half), :].astype(BF16)
    product = dot(other_head, feats)
    for t in range(tiles):
        core_out[t] = product[:, t * share : (t + 1) * share].astype(BF16)
    core_copy = pltpu.make_async_remote_copy(
        src_ref=core_out,
        dst_ref=core_in,
        send_sem=core_send,
        recv_sem=core_recv,
        device_id=(partner, me),
        device_id_type=MESH,
    )
    core_copy.start()
    product = dot(own_head, feats)
    for t in range(tiles):
        own_half[t] = product[:, t * share : (t + 1) * share]
    core_copy.wait_recv()

    tile_copies = []
    for j in order:
        dest = flipped(j)
        tile_out[j - 1] = (own_half[dest] + core_in[dest].astype(F32)).astype(BF16)
        copy = pltpu.make_async_remote_copy(
            src_ref=tile_out.at[j - 1],
            dst_ref=tile_in.at[j - 1],
            send_sem=tile_send.at[j - 1],
            recv_sem=tile_recv.at[j - 1],
            device_id=tile_peer(j),
            device_id_type=MESH,
        )
        copy.start()
        tile_copies.append(copy)
    total = own_half[me] + core_in[me].astype(F32)

    head = dot_nt(eye(pixels), head_t[...].astype(BF16)).astype(BF16)
    outputs = bins + channels
    gfeat_ref[...] = dot(head[:, :outputs], weight_ref[...]).astype(BF16)

    for k in range(1, pairs - 1):
        token_wait(k)
        if k < pairs - 2:
            token_send(k + 1)
    for at in reversed(range(tiles - 1)):
        tile_copies[at].wait_recv()
        total += tile_in[order[at] - 1].astype(F32)
    z_copies = []
    z_out[...] = total.astype(BF16)
    for j in range(1, pairs):
        copy = pltpu.make_async_remote_copy(
            src_ref=z_out,
            dst_ref=z_in.at[j - 1],
            send_sem=z_send.at[j - 1],
            recv_sem=z_recv.at[j - 1],
            device_id=z_peer(j),
            device_id_type=MESH,
        )
        copy.start()
        z_copies.append(copy)
    for j in range(1, pairs):
        z_copies[j - 1].wait_recv()
        total += z_in[j - 1].astype(F32)
    fin_out[...] = total
    fin_copy = pltpu.make_async_remote_copy(
        src_ref=fin_out,
        dst_ref=fin_in,
        send_sem=fin_send,
        recv_sem=fin_recv,
        device_id=(partner, me),
        device_id_type=MESH,
    )
    fin_copy.start()
    for copy in list(val_copies.values()) + [core_copy] + tile_copies + z_copies:
        copy.wait_send()
    fin_copy.wait()
    other = fin_in[...]
    first = core == 0
    gweight_ref[0:half, :] = jnp.where(first, total, other)
    gweight_ref[half:, :] = jnp.where(first, other, total)[: gweight_ref.shape[0] - half]


def body(tiles, dps, features, depth_probs, context, bev_grad, head_weight, slot_cell, slot_point, slot_count):
    features = features[0]
    depth_probs = depth_probs[0]
    context = context[0]
    bev_t = bev_grad[0].T
    cell_table = slot_cell[0, 0]
    points = slot_point[0, 0]
    counts = slot_count[0]
    cap = cell_table.shape[1]
    pixels, bins = depth_probs.shape
    channels = context.shape[1]
    inputs = features.shape[1]
    outputs = bins + channels
    pairs = dps // 2
    share = inputs // tiles
    half = -(-outputs // 32) * 16
    operands = (counts, features, depth_probs, context, bev_t, head_weight, cell_table, points)
    vmem = pl.BlockSpec(memory_space=pltpu.VMEM)
    dma = pltpu.SemaphoreType.DMA
    grad_feats, weight_t = pl.pallas_call(
        functools.partial(kernel, (tiles, pairs, half)),
        out_shape=(
            pltpu.VMEM((pixels, inputs), BF16),
            pltpu.VMEM((outputs, share), F32),
        ),
        in_specs=[pl.BlockSpec(memory_space=pl.ANY)] * 8,
        out_specs=(vmem, vmem),
        scratch_shapes=[pltpu.VMEM(a.shape, a.dtype) for a in operands]
        + [
            pltpu.VMEM((tiles - 1, channels, cap), BF16),
            pltpu.VMEM((tiles - 1, channels, cap), BF16),
            pltpu.VMEM((2 * half, pixels), F32),
            pltpu.VMEM((tiles, half, share), F32),
            pltpu.VMEM((tiles, half, share), BF16),
            pltpu.VMEM((tiles, half, share), BF16),
            pltpu.VMEM((tiles - 1, half, share), BF16),
            pltpu.VMEM((tiles - 1, half, share), BF16),
            pltpu.VMEM((half, share), BF16),
            pltpu.VMEM((pairs - 1, half, share), BF16),
            pltpu.VMEM((half, share), F32),
            pltpu.VMEM((half, share), F32),
            dma((len(operands),)),
            dma((tiles - 1,)),
            dma((tiles - 1,)),
            dma,
            dma,
            dma((tiles - 1,)),
            dma((tiles - 1,)),
            dma((pairs - 1,)),
            dma((pairs - 1,)),
            dma,
            dma,
            pltpu.SemaphoreType.REGULAR((max(pairs - 2, 1),)),
            pltpu.SemaphoreType.REGULAR((max(pairs - 2, 1),)),
        ],
        compiler_params=pltpu.CompilerParams(collective_id=0, has_side_effects=True),
        name="splat_backward",
    )(*operands)
    return (grad_feats[None], weight_t.T)


def solution(mesh):
    return jax.shard_map(
        functools.partial(body, mesh.shape["tile"], mesh.shape["dp"]),
        mesh=mesh,
        in_specs=(
            P("dp", "tile", None),
            P("dp", "tile", None),
            P("dp", "tile", None),
            P("dp", "tile", None),
            P(),
            P("dp", "tile", None, None),
            P("dp", "tile", None, None),
            P("dp", None, None),
        ),
        out_specs=(P("dp", "tile", None), P("tile", None)),
        check_vma=False,
    )
```
